512 devices in a mesh: grp: 2 (over y), src: 16 (over z), rcv: 8 (over x), frq: 2 (over core).
Axes of the slice: x: 8, y: 2, z: 16, core: 2. Of those that a mesh axis runs over, the one named last changes fastest.
The devices are a block of a 8x8x16 slice.
Arguments:
- left_strip: bfloat16 [4, 2, 1024, 20480], P(('grp', 'frq'), None, 'src', 'rcv'), parts along dimension 0, may hold values from -0.03125 to 0.03125
- right_strip: bfloat16 [4, 2, 1536, 20480], P(('grp', 'frq'), None, 'src', 'rcv'), parts along dimension 0, may hold values from -6 to 6
- panel_order: int32 [40], P('rcv'), may hold values from 0 to 39, as said below
- freq_slice: int32 [4], P(('grp', 'frq')), parts along dimension 0, may hold values from 0 to 63
- wavelet: float32 [64, 2], replicated, may hold values from -4 to 4
Outputs:
- multiple: float32 [4, 2, 1536, 1024], P(('grp', 'frq'), None, 'src', 'rcv'), parts along dimension 0
The draws below stay inside these ranges and needn't reach their ends.
There are 2 independent parts, one for each index of `grp`. The reference program is written for one: setup_inputs(seed, part) draws one part's arguments, and reference() takes and returns one part's arrays. A program takes and returns all parts, laid end to end along the dimension named above; an argument that names none is the same for every part. Nothing has to cross between parts.
Inputs may be any that keep to these rules, and one draw needn't show every extreme that they name: `panel_order`: each aligned block of 5 entries is a permutation of that block's own positions.
All inputs are finite; a program needn't handle non-finite values.
Results may differ from the reference program's by a relative error of at most 0.0003.
Values may be sent and summed in bfloat16 or wider, within the bound.
No kernel may reach another device: no remote copies, remote signals or barrier semaphores. Data moves between devices by JAX's collectives and lax.ppermute only.
A program may use at most 64 MiB of HBM per device.

```python
import jax
import jax.numpy as jnp
from jax import lax

PANELS_DEV = 5
NFTAB = 64
FREQS = 2
NPANELS = 40
NJ = 20480
IALL = 1024
KALL = 1536


def draw_panel_order(key, part):
    blocks_count = NPANELS // PANELS_DEV
    scores = jax.random.randint(key, (blocks_count, PANELS_DEV), 0, 1 << 20) * PANELS_DEV + jnp.arange(PANELS_DEV)[None, :]
    ranking = jnp.argsort(scores, axis=1, stable=True).astype(jnp.int32)
    offsets = (PANELS_DEV * jnp.arange(blocks_count)[:, None]).astype(jnp.int32)
    return (ranking + offsets).reshape(-1).astype(jnp.int32)


def levels(key, shape, cuts, smallest, top_value):
    def one(position, blocks):
        draws = jax.random.uniform(jax.random.fold_in(jax.random.fold_in(key, 6), position), (blocks,), jnp.float32, smallest / len(cuts), top_value / len(cuts))
        return jnp.repeat(jnp.exp(draws), shape[position] // blocks).reshape((-1,) + (1,) * (len(shape) - position - 1))

    loudness = one(*cuts[0])
    for cut in cuts[1:]:
        loudness = loudness * one(*cut)
    return loudness


def normal_values(stream_key, shape, scale, limit, split=(), held_as=jnp.bfloat16):
    entries = jax.random.normal(stream_key, shape, jnp.float32) * scale
    if len(split) > 0:
        entries = levels(stream_key, shape, split, -0.22, 0.18) * entries
    return jnp.clip(entries, min=-limit, max=limit).astype(held_as)


def setup_inputs(seed: int = 0, part: int = 0) -> dict:
    key_of = jax.random.split(jax.random.key(seed), 6)
    own_keys = jax.random.split(jax.random.fold_in(key_of[5], part), 6)
    left_strip = normal_values(own_keys[0], (FREQS, 2, IALL, NJ), (2 * NJ) ** -0.5, 0.03125, ((0, 2), (2, 16), (3, 8)))
    right_strip = normal_values(own_keys[1], (FREQS, 2, KALL, NJ), 1.0, 6.0, ((0, 2), (2, 16), (3, 8)))
    panel_order = draw_panel_order(jax.random.fold_in(key_of[5], 71), part)
    freq_slice = jax.random.randint(own_keys[3], (FREQS,), 0, NFTAB).astype(jnp.int32)
    wavelet = normal_values(key_of[4], (NFTAB, 2), 1.0, 4.0, (), jnp.float32)
    return dict(left_strip=left_strip, right_strip=right_strip, panel_order=panel_order, freq_slice=freq_slice, wavelet=wavelet)


def product(first_op, second_op):
    return jnp.dot(first_op, second_op.T, precision=lax.Precision.HIGHEST, preferred_element_type=jnp.float32)


def reference(left_strip, right_strip, panel_order, freq_slice, wavelet):
    count = panel_order.shape[0]
    receivers = left_strip.shape[2]
    results = []
    for slice_index in range(left_strip.shape[0]):
        left_part = left_strip[slice_index].astype(jnp.float32).reshape(2, receivers, count, -1)
        left_part = jnp.take(left_part, panel_order, axis=2).reshape(2, receivers, -1)
        right_part = right_strip[slice_index].astype(jnp.float32)
        real_part = product(right_part[0], left_part[0]) - product(right_part[1], left_part[1])
        imag_part = product(right_part[0], left_part[1]) + product(right_part[1], left_part[0])
        weight = wavelet[freq_slice[slice_index]]
        out_real = weight[0] * real_part - weight[1] * imag_part
        out_imag = weight[0] * imag_part + weight[1] * real_part
        results.append(jnp.stack([out_real, out_imag], 0))
    return jnp.stack(results, 0)
```

```python
import functools

import jax
import jax.numpy as jnp
from jax import lax
from jax.experimental import pallas as pl
from jax.experimental.pallas import tpu as pltpu
from jax.sharding import PartitionSpec as P

CHUNKS = 2
EARLY = 5
VMEM = pltpu.VMEM
SMEM = pltpu.SMEM


def ring_gather(block, axis, extra_up):
    n = lax.axis_size(axis)
    up = [(i, (i + 1) % n) for i in range(n)]
    down = [(i, (i - 1) % n) for i in range(n)]
    n_up = n // 2 if extra_up else n - 1 - n // 2
    n_down = n - 1 - n_up
    blocks = {0: block}
    a = b = block
    for step in range(1, n // 2 + 1):
        if step <= n_down:
            b = lax.ppermute(b, axis, down)
            blocks[step] = b
        if step <= n_up:
            a = lax.ppermute(a, axis, up)
            blocks[n - step] = a
    return blocks


def order_kernel(order, right, out):
    panels = order.shape[0]
    sources, positions = right.shape[2], right.shape[3]
    width = positions // panels
    for p in range(panels):
        target = pl.multiple_of(lax.rem(order[p], panels) * width, width)
        for part in range(2):
            out[pl.ds(part * sources, sources), pl.ds(target, width)] = right[
                0, part, :, pl.ds(p * width, width)
            ]


def product_kernel(relative, n, per, aliased, place, right, *refs):
    blocks, out = refs[: len(relative)], refs[-1]
    if aliased:
        out[...] = refs[-2][...]
    rows = blocks[0].shape[1]
    sources = right.shape[0] // 2

    def with_part(part):
        left = jnp.concatenate([block[part] for block in blocks], axis=0)
        return lax.dot_general(
            right[...], left, (((1,), (1,)), ((), ())), preferred_element_type=jnp.float32
        )

    by_real, by_imag = with_part(0), with_part(1)
    real = by_real[:sources] - by_imag[sources:]
    imag = by_imag[:sources] + by_real[sources:]
    for i, r in enumerate(relative):
        tile = lax.rem(place[0] + r, n) // per
        piece = jnp.concatenate(
            [real[:, i * rows : (i + 1) * rows], imag[:, i * rows : (i + 1) * rows]], axis=1
        )
        out[tile, :, pl.ds((r % per) * 2 * rows, 2 * rows)] = piece


def product(place, right, blocks, relative, n, m, before):
    rows = blocks[0].shape[1]
    sources = right.shape[0] // 2
    per = n // m
    operands = [place, right, *blocks]
    specs = [pl.BlockSpec(memory_space=SMEM)] + [pl.BlockSpec(memory_space=VMEM)] * (len(operands) - 1)
    aliases = {}
    if before is not None:
        aliases = {len(operands): 0}
        operands.append(before)
        specs.append(pl.BlockSpec(memory_space=VMEM))
    return pl.pallas_call(
        functools.partial(product_kernel, relative, n, per, before is not None),
        out_shape=jax.ShapeDtypeStruct((m, sources, per * 2 * rows), jnp.float32),
        in_specs=specs,
        out_specs=pl.BlockSpec(memory_space=VMEM),
        input_output_aliases=aliases,
        name="product",
    )(*operands)


def finish_kernel(place, slice_of, wavelet, *refs):
    arrived, out = refs[:-1], refs[-1]
    lanes = arrived[0].shape[2]
    rows = lanes // 4
    odd = lax.rem(place[0], 2) == 1
    sums = [ref[...].sum(axis=0) for ref in arrived]

    def lay(part):
        halves = [
            jnp.concatenate(
                [s[:, (2 * h + part) * rows : (2 * h + part + 1) * rows] for s in sums], axis=1
            )
            for h in range(2)
        ]
        return jnp.concatenate(
            [jnp.where(odd, halves[1], halves[0]), jnp.where(odd, halves[0], halves[1])], axis=1
        )

    real, imag = lay(0), lay(1)
    index = slice_of[0]
    weight_real, weight_imag = wavelet[index, 0], wavelet[index, 1]
    out[0, 0] = weight_real * real - weight_imag * imag
    out[0, 1] = weight_real * imag + weight_imag * real


def local(left_strip, right_strip, panel_order, freq_slice, wavelet):
    _, _, receivers, positions = left_strip.shape
    sources = right_strip.shape[2]
    n, m = lax.axis_size("src"), lax.axis_size("rcv")
    place = lax.axis_index("src").astype(jnp.int32).reshape(1)
    right = pl.pallas_call(
        order_kernel,
        out_shape=jax.ShapeDtypeStruct((2 * sources, positions), jnp.bfloat16),
        in_specs=[pl.BlockSpec(memory_space=SMEM), pl.BlockSpec(memory_space=VMEM)],
        out_specs=pl.BlockSpec(memory_space=VMEM),
        name="order",
    )(panel_order, right_strip)
    rows = receivers // CHUNKS
    gathered = [
        ring_gather(left_strip[0, :, c * rows : (c + 1) * rows], "src", c % 2 == 0)
        for c in range(CHUNKS)
    ]
    arrived = []
    for blocks in gathered:
        first = [r for r in range(n) if min(r, n - r) <= EARLY]
        last = [r for r in range(n) if min(r, n - r) > EARLY]
        tiles = product(place, right, [blocks[r] for r in first], first, n, m, None)
        tiles = product(place, right, [blocks[r] for r in last], last, n, m, tiles)
        arrived.append(lax.all_to_all(tiles, "rcv", split_axis=0, concat_axis=0, tiled=True))
    return pl.pallas_call(
        finish_kernel,
        out_shape=jax.ShapeDtypeStruct((1, 2, sources, n * receivers // m), jnp.float32),
        in_specs=[pl.BlockSpec(memory_space=SMEM)] * 3 + [pl.BlockSpec(memory_space=VMEM)] * CHUNKS,
        out_specs=pl.BlockSpec(memory_space=VMEM),
        name="finish",
    )(place, freq_slice, wavelet, *arrived)


def solution(mesh):
    placed = (
        P(("grp", "frq"), None, "src", "rcv"),
        P(("grp", "frq"), None, "src", "rcv"),
        P("rcv"),
        P(("grp", "frq")),
        P(),
    )
    return jax.shard_map(
        local,
        mesh=mesh,
        in_specs=placed,
        out_specs=P(("grp", "frq"), None, "src", "rcv"),
        check_vma=False,
    )
```

```python
import functools

import jax
import jax.numpy as jnp
from jax import lax
from jax.experimental import pallas as pl
from jax.experimental.pallas import tpu as pltpu
from jax.sharding import PartitionSpec as P

CHUNKS = 1
STAGGER = 400
UDELAY = 700
PRODUCT_VMEM = 24 << 20
SMALL_VMEM = 8 << 20
VMEM = pltpu.VMEM
SMEM = pltpu.SMEM


def wait_kernel(first, second, core, _, spun):
    turns = jnp.where(core[0] == 0, first, second)
    spun[...] = lax.fori_loop(0, turns, lambda _, x: x * 0.5 + 1.0, jnp.zeros((8, 128), jnp.float32))


def wait(core, after, first, second):
    return pl.pallas_call(
        functools.partial(wait_kernel, first, second),
        out_shape=jax.ShapeDtypeStruct((8, 128), jnp.float32),
        in_specs=[pl.BlockSpec(memory_space=SMEM), pl.BlockSpec(memory_space=VMEM)],
        out_specs=pl.BlockSpec(memory_space=VMEM),
        compiler_params=pltpu.CompilerParams(vmem_limit_bytes=SMALL_VMEM),
        name="wait",
    )(core, after)


def order_kernel(order, right, _, out):
    panels = order.shape[0]
    sources, positions = right.shape[2], right.shape[3]
    width = positions // panels
    for p in range(panels):
        target = pl.multiple_of(lax.rem(order[p], panels) * width, width)
        for part in range(2):
            out[pl.ds(part * sources, sources), pl.ds(target, width)] = right[
                0, part, :, pl.ds(p * width, width)
            ]


def multiply(right, blocks):
    rows = blocks[0].shape[1]
    sources = right.shape[0] // 2

    def with_part(part):
        left = jnp.concatenate([block[part] for block in blocks], axis=0)
        return lax.dot_general(
            right[...], left, (((1,), (1,)), ((), ())), preferred_element_type=jnp.float32
        )

    by_real, by_imag = with_part(0), with_part(1)
    real = by_real[:sources] - by_imag[sources:]
    imag = by_imag[:sources] + by_real[sources:]
    return [
        jnp.concatenate(
            [real[:, i * rows : (i + 1) * rows], imag[:, i * rows : (i + 1) * rows]], axis=1
        )
        for i in range(len(blocks))
    ]


def product_kernel(right, *refs):
    for i, piece in enumerate(multiply(right, refs[:-1])):
        refs[-1][i] = piece


def product(right, blocks):
    rows = blocks[0].shape[1]
    return pl.pallas_call(
        product_kernel,
        out_shape=jax.ShapeDtypeStruct((len(blocks), right.shape[0] // 2, 2 * rows), jnp.float32),
        in_specs=[pl.BlockSpec(memory_space=VMEM)] * (1 + len(blocks)),
        out_specs=pl.BlockSpec(memory_space=VMEM),
        compiler_params=pltpu.CompilerParams(vmem_limit_bytes=PRODUCT_VMEM),
        name="product",
    )(right, *blocks)


def assemble_kernel(early, late, n, per, place, right, *refs):
    out = refs[-1]
    blocks = refs[len(early) : -1]

    def store(r, piece):
        lanes = piece.shape[1]
        out[lax.rem(place[0] + r, n) // per, :, pl.ds((r % per) * lanes, lanes)] = piece

    for relative, pieces in zip(early, refs):
        for i, r in enumerate(relative):
            store(r, pieces[i])
    for r, piece in zip(late, multiply(right, blocks)):
        store(r, piece)


def assemble(place, right, early, pieces, late, blocks, n, m):
    rows = blocks[0].shape[1]
    per = n // m
    return pl.pallas_call(
        functools.partial(assemble_kernel, early, late, n, per),
        out_shape=jax.ShapeDtypeStruct((m, right.shape[0] // 2, per * 2 * rows), jnp.float32),
        in_specs=[pl.BlockSpec(memory_space=SMEM)]
        + [pl.BlockSpec(memory_space=VMEM)] * (1 + len(pieces) + len(blocks)),
        out_specs=pl.BlockSpec(memory_space=VMEM),
        compiler_params=pltpu.CompilerParams(vmem_limit_bytes=PRODUCT_VMEM),
        name="assemble",
    )(place, right, *pieces, *blocks)


def finish_kernel(place, slice_of, wavelet, *refs):
    arrived, out = refs[:-1], refs[-1]
    lanes = arrived[0].shape[2]
    rows = lanes // 4
    odd = lax.rem(place[0], 2) == 1
    sums = [ref[...].sum(axis=0) for ref in arrived]

    def lay(part):
        halves = [
            jnp.concatenate(
                [s[:, (2 * h + part) * rows : (2 * h + part + 1) * rows] for s in sums], axis=1
            )
            for h in range(2)
        ]
        return jnp.concatenate(
            [jnp.where(odd, halves[1], halves[0]), jnp.where(odd, halves[0], halves[1])], axis=1
        )

    real, imag = lay(0), lay(1)
    index = slice_of[0]
    weight_real, weight_imag = wavelet[0, index], wavelet[1, index]
    out[0, 0] = weight_real * real - weight_imag * imag
    out[0, 1] = weight_real * imag + weight_imag * real


def local(left_strip, right_strip, panel_order, freq_slice, wavelet):
    _, _, receivers, positions = left_strip.shape
    sources = right_strip.shape[2]
    n, m = lax.axis_size("src"), lax.axis_size("rcv")
    place = lax.axis_index("src").astype(jnp.int32).reshape(1)
    core = lax.axis_index("frq").astype(jnp.int32).reshape(1)
    spun = wait(core, jnp.zeros((8, 128), jnp.float32), STAGGER, 0)
    left_strip, spun = lax.optimization_barrier((left_strip, spun))
    right = pl.pallas_call(
        order_kernel,
        out_shape=jax.ShapeDtypeStruct((2 * sources, positions), jnp.bfloat16),
        in_specs=[
            pl.BlockSpec(memory_space=SMEM),
            pl.BlockSpec(memory_space=VMEM),
            pl.BlockSpec(memory_space=VMEM),
        ],
        out_specs=pl.BlockSpec(memory_space=VMEM),
        compiler_params=pltpu.CompilerParams(vmem_limit_bytes=SMALL_VMEM),
        name="order",
    )(panel_order, right_strip, spun)
    up = [(i, (i + 1) % n) for i in range(n)]
    down = [(i, (i - 1) % n) for i in range(n)]
    half = n // 2
    own = left_strip[0]
    pieces, early = [product(right, [own])], [(0,)]
    spun = wait(core, pieces[0][0, :8, :], UDELAY, UDELAY)
    low, pieces[0], spun = lax.optimization_barrier((own, pieces[0], spun))
    from_above, from_below = lax.ppermute(own, "src", down), lax.ppermute(low, "src", up)
    held = {1: from_above, n - 1: from_below}
    for step in range(2, half + 1):
        from_above = lax.ppermute(from_above, "src", down)
        if step < half:
            from_below = lax.ppermute(from_below, "src", up)
            pieces.append(product(right, list(held.values())))
            early.append(tuple(held))
            from_above, pieces[-1] = lax.optimization_barrier((from_above, pieces[-1]))
            held = {step: from_above, n - step: from_below}
    held[half] = from_above
    tiles = assemble(place, right, early, pieces, tuple(held), list(held.values()), n, m)
    arrived = [lax.all_to_all(tiles, "rcv", split_axis=0, concat_axis=0, tiled=True)]
    return pl.pallas_call(
        finish_kernel,
        out_shape=jax.ShapeDtypeStruct((1, 2, sources, n * receivers // m), jnp.float32),
        in_specs=[pl.BlockSpec(memory_space=SMEM)] * 3 + [pl.BlockSpec(memory_space=VMEM)] * CHUNKS,
        out_specs=pl.BlockSpec(memory_space=VMEM),
        compiler_params=pltpu.CompilerParams(vmem_limit_bytes=SMALL_VMEM),
        name="finish",
    )(place, freq_slice, wavelet.T, *arrived)


def solution(mesh):
    placed = (
        P(("grp", "frq"), None, "src", "rcv"),
        P(("grp", "frq"), None, "src", "rcv"),
        P("rcv"),
        P(("grp", "frq")),
        P(),
    )
    return jax.shard_map(
        local,
        mesh=mesh,
        in_specs=placed,
        out_specs=P(("grp", "frq"), None, "src", "rcv"),
        check_vma=False,
    )
```

```python
import functools

import jax
import jax.numpy as jnp
from jax import lax
from jax.experimental import pallas as pl
from jax.experimental.pallas import tpu as pltpu
from jax.sharding import PartitionSpec as P


CHUNKS = 2
PRODUCT_STEPS = (3, 6)
PRODUCT_VMEM = 24 << 20
SMALL_VMEM = 8 << 20
VMEM = pltpu.VMEM
SMEM = pltpu.SMEM


def order_kernel(order, right, out):
    panels = order.shape[0]
    sources, positions = right.shape[2], right.shape[3]
    width = positions // panels
    for p in range(panels):
        target = pl.multiple_of(lax.rem(order[p], panels) * width, width)
        for part in range(2):
            out[pl.ds(part * sources, sources), pl.ds(target, width)] = right[
                0, part, :, pl.ds(p * width, width)
            ]


def multiply(right, refs):
    rows = refs[0].shape[1] * CHUNKS
    sources = right.shape[0] // 2

    def with_part(part):
        left = jnp.concatenate([ref[part] for ref in refs], axis=0)
        return lax.dot_general(
            right[...], left, (((1,), (1,)), ((), ())), preferred_element_type=jnp.float32
        )

    by_real, by_imag = with_part(0), with_part(1)
    real = by_real[:sources] - by_imag[sources:]
    imag = by_imag[:sources] + by_real[sources:]
    return [
        jnp.concatenate(
            [real[:, i * rows : (i + 1) * rows], imag[:, i * rows : (i + 1) * rows]], axis=1
        )
        for i in range(len(refs) // CHUNKS)
    ]


def product_kernel(right, *refs):
    for i, piece in enumerate(multiply(right, refs[:-1])):
        refs[-1][i] = piece


def flat(held):
    return [chunk for block in held.values() for chunk in block]


def product(right, held):
    rows = sum(chunk.shape[1] for chunk in next(iter(held.values())))
    operands = [right, *flat(held)]
    return pl.pallas_call(
        product_kernel,
        out_shape=jax.ShapeDtypeStruct((len(held), right.shape[0] // 2, 2 * rows), jnp.float32),
        in_specs=[pl.BlockSpec(memory_space=VMEM)] * len(operands),
        out_specs=pl.BlockSpec(memory_space=VMEM),
        compiler_params=pltpu.CompilerParams(vmem_limit_bytes=PRODUCT_VMEM),
        name="product",
    )(*operands)


def assemble_kernel(early, late, n, per, place, right, *refs):
    out = refs[-1]

    def store(r, piece):
        lanes = piece.shape[1]
        out[lax.rem(place[0] + r, n) // per, :, pl.ds((r % per) * lanes, lanes)] = piece

    for relative, pieces in zip(early, refs):
        for i, r in enumerate(relative):
            store(r, pieces[i])
    for r, piece in zip(late, multiply(right, refs[len(early) : -1])):
        store(r, piece)


def assemble(place, right, early, pieces, held, n, m):
    lanes = pieces[0].shape[2]
    per = n // m
    operands = [right, *pieces, *flat(held)]
    return pl.pallas_call(
        functools.partial(assemble_kernel, early, tuple(held), n, per),
        out_shape=jax.ShapeDtypeStruct((m, right.shape[0] // 2, per * lanes), jnp.float32),
        in_specs=[pl.BlockSpec(memory_space=SMEM)]
        + [pl.BlockSpec(memory_space=VMEM)] * len(operands),
        out_specs=pl.BlockSpec(memory_space=VMEM),
        compiler_params=pltpu.CompilerParams(vmem_limit_bytes=PRODUCT_VMEM),
        name="assemble",
    )(place, *operands)


def finish_kernel(place, slice_of, wavelet, *refs):
    arrived, out = refs[:-1], refs[-1]
    lanes = arrived[0].shape[2]
    rows = lanes // 4
    odd = lax.rem(place[0], 2) == 1
    sums = [ref[...].sum(axis=0) for ref in arrived]

    def lay(part):
        halves = [
            jnp.concatenate(
                [s[:, (2 * h + part) * rows : (2 * h + part + 1) * rows] for s in sums], axis=1
            )
            for h in range(2)
        ]
        return jnp.concatenate(
            [jnp.where(odd, halves[1], halves[0]), jnp.where(odd, halves[0], halves[1])], axis=1
        )

    real, imag = lay(0), lay(1)
    index = slice_of[0]
    weight_real, weight_imag = wavelet[0, index], wavelet[1, index]
    out[0, 0] = weight_real * real - weight_imag * imag
    out[0, 1] = weight_real * imag + weight_imag * real


def local(left_strip, right_strip, panel_order, freq_slice, wavelet):
    _, _, receivers, positions = left_strip.shape
    sources = right_strip.shape[2]
    n, m = lax.axis_size("src"), lax.axis_size("rcv")
    place = lax.axis_index("src").astype(jnp.int32).reshape(1)
    right = pl.pallas_call(
        order_kernel,
        out_shape=jax.ShapeDtypeStruct((2 * sources, positions), jnp.bfloat16),
        in_specs=[
            pl.BlockSpec(memory_space=SMEM),
            pl.BlockSpec(memory_space=VMEM),
        ],
        out_specs=pl.BlockSpec(memory_space=VMEM),
        compiler_params=pltpu.CompilerParams(vmem_limit_bytes=SMALL_VMEM),
        name="order",
    )(panel_order, right_strip)
    up = [(i, (i + 1) % n) for i in range(n)]
    down = [(i, (i - 1) % n) for i in range(n)]
    half = n // 2
    rows = receivers // CHUNKS
    own = [left_strip[0, :, c * rows : (c + 1) * rows] for c in range(CHUNKS)]
    above, below = list(own), list(own)
    held = {0: tuple(own)}
    pieces, early = [], []
    for step in range(1, half + 1):
        if step in PRODUCT_STEPS:
            pieces.append(product(right, held))
            early.append(tuple(held))
            held = {}
        for c in range(CHUNKS):
            above[c] = lax.ppermute(above[c], "src", down)
            if step < half:
                below[c] = lax.ppermute(below[c], "src", up)
        held[step] = tuple(above)
        if step < half:
            held[n - step] = tuple(below)
    tiles = assemble(place, right, early, pieces, held, n, m)
    arrived = [lax.all_to_all(tiles, "rcv", split_axis=0, concat_axis=0, tiled=True)]
    return pl.pallas_call(
        finish_kernel,
        out_shape=jax.ShapeDtypeStruct((1, 2, sources, n * receivers // m), jnp.float32),
        in_specs=[pl.BlockSpec(memory_space=SMEM)] * 3 + [pl.BlockSpec(memory_space=VMEM)],
        out_specs=pl.BlockSpec(memory_space=VMEM),
        compiler_params=pltpu.CompilerParams(vmem_limit_bytes=SMALL_VMEM),
        name="finish",
    )(place, freq_slice, wavelet.T, *arrived)


def solution(mesh):
    placed = (
        P(("grp", "frq"), None, "src", "rcv"),
        P(("grp", "frq"), None, "src", "rcv"),
        P("rcv"),
        P(("grp", "frq")),
        P(),
    )
    return jax.shard_map(
        local,
        mesh=mesh,
        in_specs=placed,
        out_specs=P(("grp", "frq"), None, "src", "rcv"),
        check_vma=False,
    )
```

```python
import functools

import jax
import jax.numpy as jnp
from jax import lax
from jax.experimental import pallas as pl
from jax.experimental.pallas import tpu as pltpu
from jax.sharding import PartitionSpec as P


CHUNKS = 2
PRODUCT_STEPS = (3, 6, 8)
PRODUCT_VMEM = 24 << 20
SMALL_VMEM = 8 << 20
VMEM = pltpu.VMEM
SMEM = pltpu.SMEM


def order_kernel(order, right, out):
    panels = order.shape[0]
    sources, positions = right.shape[2], right.shape[3]
    width = positions // panels
    for p in range(panels):
        target = pl.multiple_of(lax.rem(order[p], panels) * width, width)
        for part in range(2):
            out[pl.ds(part * sources, sources), pl.ds(target, width)] = right[
                0, part, :, pl.ds(p * width, width)
            ]


def multiply(right, refs):
    rows = refs[0].shape[1] * CHUNKS
    sources = right.shape[0] // 2

    def with_part(part):
        left = jnp.concatenate([ref[part] for ref in refs], axis=0)
        return lax.dot_general(
            right[...], left, (((1,), (1,)), ((), ())), preferred_element_type=jnp.float32
        )

    by_real, by_imag = with_part(0), with_part(1)
    real = by_real[:sources] - by_imag[sources:]
    imag = by_imag[:sources] + by_real[sources:]
    return [
        jnp.concatenate(
            [real[:, i * rows : (i + 1) * rows], imag[:, i * rows : (i + 1) * rows]], axis=1
        )
        for i in range(len(refs) // CHUNKS)
    ]


def product_kernel(right, *refs):
    for i, piece in enumerate(multiply(right, refs[:-1])):
        refs[-1][i] = piece


def flat(held):
    return [chunk for block in held.values() for chunk in block]


def product(right, held):
    rows = sum(chunk.shape[1] for chunk in next(iter(held.values())))
    operands = [right, *flat(held)]
    return pl.pallas_call(
        product_kernel,
        out_shape=jax.ShapeDtypeStruct((len(held), right.shape[0] // 2, 2 * rows), jnp.float32),
        in_specs=[pl.BlockSpec(memory_space=VMEM)] * len(operands),
        out_specs=pl.BlockSpec(memory_space=VMEM),
        compiler_params=pltpu.CompilerParams(vmem_limit_bytes=PRODUCT_VMEM),
        name="product",
    )(*operands)


def assemble_kernel(early, late, n, per, place, right, *refs):
    out = refs[-1]

    def store(r, piece):
        lanes = piece.shape[1]
        out[lax.rem(place[0] + r, n) // per, :, pl.ds((r % per) * lanes, lanes)] = piece

    for relative, pieces in zip(early, refs):
        for i, r in enumerate(relative):
            store(r, pieces[i])
    for r, piece in zip(late, multiply(right, refs[len(early) : -1])):
        store(r, piece)


def assemble(place, right, early, pieces, held, n, m):
    lanes = pieces[0].shape[2]
    per = n // m
    operands = [right, *pieces, *flat(held)]
    return pl.pallas_call(
        functools.partial(assemble_kernel, early, tuple(held), n, per),
        out_shape=jax.ShapeDtypeStruct((m, right.shape[0] // 2, per * lanes), jnp.float32),
        in_specs=[pl.BlockSpec(memory_space=SMEM)]
        + [pl.BlockSpec(memory_space=VMEM)] * len(operands),
        out_specs=pl.BlockSpec(memory_space=VMEM),
        compiler_params=pltpu.CompilerParams(vmem_limit_bytes=PRODUCT_VMEM),
        name="assemble",
    )(place, *operands)


def finish_kernel(place, slice_of, wavelet, *refs):
    arrived, out = refs[:-1], refs[-1]
    lanes = arrived[0].shape[2]
    rows = lanes // 4
    odd = lax.rem(place[0], 2) == 1
    sums = [ref[...].sum(axis=0) for ref in arrived]

    def lay(part):
        halves = [
            jnp.concatenate(
                [s[:, (2 * h + part) * rows : (2 * h + part + 1) * rows] for s in sums], axis=1
            )
            for h in range(2)
        ]
        return jnp.concatenate(
            [jnp.where(odd, halves[1], halves[0]), jnp.where(odd, halves[0], halves[1])], axis=1
        )

    real, imag = lay(0), lay(1)
    index = slice_of[0]
    weight_real, weight_imag = wavelet[0, index], wavelet[1, index]
    out[0, 0] = weight_real * real - weight_imag * imag
    out[0, 1] = weight_real * imag + weight_imag * real


def local(left_strip, right_strip, panel_order, freq_slice, wavelet):
    _, _, receivers, positions = left_strip.shape
    sources = right_strip.shape[2]
    n, m = lax.axis_size("src"), lax.axis_size("rcv")
    place = lax.axis_index("src").astype(jnp.int32).reshape(1)
    right = pl.pallas_call(
        order_kernel,
        out_shape=jax.ShapeDtypeStruct((2 * sources, positions), jnp.bfloat16),
        in_specs=[
            pl.BlockSpec(memory_space=SMEM),
            pl.BlockSpec(memory_space=VMEM),
        ],
        out_specs=pl.BlockSpec(memory_space=VMEM),
        compiler_params=pltpu.CompilerParams(vmem_limit_bytes=SMALL_VMEM),
        name="order",
    )(panel_order, right_strip)
    up = [(i, (i + 1) % n) for i in range(n)]
    down = [(i, (i - 1) % n) for i in range(n)]
    half = n // 2
    rows = receivers // CHUNKS
    own = [left_strip[0, :, c * rows : (c + 1) * rows] for c in range(CHUNKS)]
    above, below = list(own), list(own)
    held = {0: tuple(own)}
    pieces, early = [], []
    for step in range(1, half + 1):
        if step in PRODUCT_STEPS:
            pieces.append(product(right, held))
            early.append(tuple(held))
            held = {}
        for c in range(CHUNKS):
            if step < half or c == 0:
                above[c] = lax.ppermute(above[c], "src", down)
            if step < half or c == 1:
                below[c] = lax.ppermute(below[c], "src", up)
        if step < half:
            held[step] = tuple(above)
            held[n - step] = tuple(below)
        else:
            held[step] = (above[0], below[1])
    tiles = assemble(place, right, early, pieces, held, n, m)
    arrived = [lax.all_to_all(tiles, "rcv", split_axis=0, concat_axis=0, tiled=True)]
    return pl.pallas_call(
        finish_kernel,
        out_shape=jax.ShapeDtypeStruct((1, 2, sources, n * receivers // m), jnp.float32),
        in_specs=[pl.BlockSpec(memory_space=SMEM)] * 3 + [pl.BlockSpec(memory_space=VMEM)],
        out_specs=pl.BlockSpec(memory_space=VMEM),
        compiler_params=pltpu.CompilerParams(vmem_limit_bytes=SMALL_VMEM),
        name="finish",
    )(place, freq_slice, wavelet.T, *arrived)


def solution(mesh):
    placed = (
        P(("grp", "frq"), None, "src", "rcv"),
        P(("grp", "frq"), None, "src", "rcv"),
        P("rcv"),
        P(("grp", "frq")),
        P(),
    )
    return jax.shard_map(
        local,
        mesh=mesh,
        in_specs=placed,
        out_specs=P(("grp", "frq"), None, "src", "rcv"),
        check_vma=False,
    )
```

```python
import functools

import jax
import jax.numpy as jnp
from jax import lax
from jax.experimental import pallas as pl
from jax.experimental.pallas import tpu as pltpu
from jax.sharding import PartitionSpec as P


CHUNKS = 2
PRODUCT_STEPS = (3, 6, 7, 8)
PRODUCT_VMEM = 24 << 20
SMALL_VMEM = 8 << 20
VMEM = pltpu.VMEM
SMEM = pltpu.SMEM


def order_kernel(order, right, out):
    panels = order.shape[0]
    sources, positions = right.shape[2], right.shape[3]
    width = positions // panels
    for p in range(panels):
        target = pl.multiple_of(lax.rem(order[p], panels) * width, width)
        for part in range(2):
            out[pl.ds(part * sources, sources), pl.ds(target, width)] = right[
                0, part, :, pl.ds(p * width, width)
            ]


def multiply(right, refs):
    rows = refs[0].shape[1] * CHUNKS
    sources = right.shape[0] // 2

    def with_part(part):
        left = jnp.concatenate([ref[part] for ref in refs], axis=0)
        return lax.dot_general(
            right[...], left, (((1,), (1,)), ((), ())), preferred_element_type=jnp.float32
        )

    by_real, by_imag = with_part(0), with_part(1)
    real = by_real[:sources] - by_imag[sources:]
    imag = by_imag[:sources] + by_real[sources:]
    return [
        jnp.concatenate(
            [real[:, i * rows : (i + 1) * rows], imag[:, i * rows : (i + 1) * rows]], axis=1
        )
        for i in range(len(refs) // CHUNKS)
    ]


def product_kernel(right, *refs):
    for i, piece in enumerate(multiply(right, refs[:-1])):
        refs[-1][i] = piece


def flat(held):
    return [chunk for block in held.values() for chunk in block]


def product(right, held):
    rows = sum(chunk.shape[1] for chunk in next(iter(held.values())))
    operands = [right, *flat(held)]
    return pl.pallas_call(
        product_kernel,
        out_shape=jax.ShapeDtypeStruct((len(held), right.shape[0] // 2, 2 * rows), jnp.float32),
        in_specs=[pl.BlockSpec(memory_space=VMEM)] * len(operands),
        out_specs=pl.BlockSpec(memory_space=VMEM),
        compiler_params=pltpu.CompilerParams(vmem_limit_bytes=PRODUCT_VMEM),
        name="product",
    )(*operands)


def assemble_kernel(early, n, per, place, *refs):
    out = refs[-1]
    lanes = refs[0].shape[2]

    def store(r, piece):
        out[lax.rem(place[0] + r, n) // per, :, pl.ds((r % per) * lanes, lanes)] = piece

    for relative, pieces in zip(early, refs):
        for i, r in enumerate(relative):
            store(r, pieces[i])
    store(n // 2, jnp.zeros(refs[0].shape[1:], jnp.float32))


def assemble(place, early, pieces, n, m):
    _, sources, lanes = pieces[0].shape
    per = n // m
    return pl.pallas_call(
        functools.partial(assemble_kernel, early, n, per),
        out_shape=jax.ShapeDtypeStruct((m, sources, per * lanes), jnp.float32),
        in_specs=[pl.BlockSpec(memory_space=SMEM)]
        + [pl.BlockSpec(memory_space=VMEM)] * len(pieces),
        out_specs=pl.BlockSpec(memory_space=VMEM),
        compiler_params=pltpu.CompilerParams(vmem_limit_bytes=SMALL_VMEM),
        name="assemble",
    )(place, *pieces)


def root_of(z, n, m):
    return (z + n // 2) % n // (n // m)


def shifts(m):
    return sorted(range(1, m), key=lambda s: -min(s, m - s))


def finish_kernel(place, slice_of, wavelet, arrived, own, *refs):
    out = refs[-1]
    lanes = arrived.shape[2]
    rows = lanes // 4
    odd = lax.rem(place[0], 2) == 1
    total = arrived[...].sum(axis=0)
    far = jnp.where(place[1] == 1, own[0], 0.0)
    for ref in refs[:-1]:
        far = far + ref[0]
    sums = [jnp.concatenate([total[:, : lanes // 2] + far, total[:, lanes // 2 :]], axis=1)]

    def lay(part):
        halves = [
            jnp.concatenate(
                [s[:, (2 * h + part) * rows : (2 * h + part + 1) * rows] for s in sums], axis=1
            )
            for h in range(2)
        ]
        return jnp.concatenate(
            [jnp.where(odd, halves[1], halves[0]), jnp.where(odd, halves[0], halves[1])], axis=1
        )

    real, imag = lay(0), lay(1)
    index = slice_of[0]
    weight_real, weight_imag = wavelet[0, index], wavelet[1, index]
    out[0, 0] = weight_real * real - weight_imag * imag
    out[0, 1] = weight_real * imag + weight_imag * real


def local(left_strip, right_strip, panel_order, freq_slice, wavelet):
    _, _, receivers, positions = left_strip.shape
    sources = right_strip.shape[2]
    n, m = lax.axis_size("src"), lax.axis_size("rcv")
    place = lax.axis_index("src").astype(jnp.int32).reshape(1)
    right = pl.pallas_call(
        order_kernel,
        out_shape=jax.ShapeDtypeStruct((2 * sources, positions), jnp.bfloat16),
        in_specs=[
            pl.BlockSpec(memory_space=SMEM),
            pl.BlockSpec(memory_space=VMEM),
        ],
        out_specs=pl.BlockSpec(memory_space=VMEM),
        compiler_params=pltpu.CompilerParams(vmem_limit_bytes=SMALL_VMEM),
        name="order",
    )(panel_order, right_strip)
    up = [(i, (i + 1) % n) for i in range(n)]
    down = [(i, (i - 1) % n) for i in range(n)]
    half = n // 2
    rows = receivers // CHUNKS
    own = [left_strip[0, :, c * rows : (c + 1) * rows] for c in range(CHUNKS)]
    above, below = list(own), list(own)
    held = {0: tuple(own)}
    pieces, early = [], []
    for step in range(1, half + 1):
        if step in PRODUCT_STEPS:
            pieces.append(product(right, held))
            early.append(tuple(held))
            held = {}
        for c in range(CHUNKS):
            above[c] = lax.ppermute(above[c], "src", down)
            if step < half:
                below[c] = lax.ppermute(below[c], "src", up)
        held[step] = tuple(above)
        if step < half:
            held[n - step] = tuple(below)
    tiles = assemble(place, early, pieces, n, m)
    arrived = lax.all_to_all(tiles, "rcv", split_axis=0, concat_axis=0, tiled=True)
    own_far = product(right, {half: held[half]})
    far = []
    for s in shifts(m):
        pairs = []
        for row in range(n):
            root = root_of(row, n, m)
            pairs.append((row * m + (root - s) % m, row * m + root))
        far.append(lax.ppermute(own_far, ("src", "rcv"), pairs))
    is_root = lax.axis_index("rcv") == root_of(lax.axis_index("src"), n, m)
    return pl.pallas_call(
        finish_kernel,
        out_shape=jax.ShapeDtypeStruct((1, 2, sources, n * receivers // m), jnp.float32),
        in_specs=[pl.BlockSpec(memory_space=SMEM)] * 3
        + [pl.BlockSpec(memory_space=VMEM)] * (2 + len(far)),
        out_specs=pl.BlockSpec(memory_space=VMEM),
        compiler_params=pltpu.CompilerParams(vmem_limit_bytes=SMALL_VMEM),
        name="finish",
    )(
        jnp.concatenate([place, is_root.astype(jnp.int32).reshape(1)]),
        freq_slice,
        wavelet.T,
        arrived,
        own_far,
        *far,
    )


def solution(mesh):
    placed = (
        P(("grp", "frq"), None, "src", "rcv"),
        P(("grp", "frq"), None, "src", "rcv"),
        P("rcv"),
        P(("grp", "frq")),
        P(),
    )
    return jax.shard_map(
        local,
        mesh=mesh,
        in_specs=placed,
        out_specs=P(("grp", "frq"), None, "src", "rcv"),
        check_vma=False,
    )
```
